256 devices in a mesh: data: 256 (over z, y, x, core).
Axes of the slice: x: 4, y: 4, z: 8, core: 2. Of those that a mesh axis runs over, the one named last changes fastest.
Arguments:
- tokens: bfloat16 [131072, 768], P('data')
- labels: int32 [4, 131072], P(None, 'data')
- w_one: bfloat16 [768, 3072], replicated
- w_two: bfloat16 [3072, 768], replicated
- adapter_a: bfloat16 [768, 8], replicated
- adapter_b: bfloat16 [8, 3072], replicated
- task_heads: bfloat16 [4, 768, 3], replicated
Outputs:
- output 1: float32 [4], replicated
- output 2: float32 [768, 8], P('data')
- output 3: float32 [8, 3072], P(None, 'data')
All inputs are finite; a program needn't handle non-finite values.
Results may differ from the reference program's by a relative error of at most 0.001.
Values are sent between devices in bfloat16 or wider.
A program may use at most 768 MiB of HBM per device.

```python
import jax
import jax.numpy as jnp
from jax import lax

DEVICES = 256
TOK_DEV = 512
D_MODEL = 768
D_FF = 3072
LORA_RANK = 8
NUM_TASKS = 4
NUM_CLASSES = 3
EG_STEPS = 20


def draw_labels(label_key):
    key_list = jax.random.split(label_key, 4)
    total_tok = DEVICES * TOK_DEV
    dev_shift = jax.random.randint(key_list[0], (DEVICES, 1), 0, NUM_CLASSES)
    half_width = (NUM_CLASSES + 1) // 2
    common_lab = (dev_shift + jax.random.randint(key_list[1], (DEVICES, TOK_DEV), 0, half_width)) % NUM_CLASSES
    common_lab = common_lab.reshape(total_tok)
    own_lab = jax.random.randint(key_list[2], (NUM_TASKS, total_tok), 0, NUM_CLASSES)
    pick_common = jax.random.randint(key_list[3], (NUM_TASKS, total_tok), 0, 5) < 3
    return jnp.where(pick_common, common_lab[None, :], own_lab).astype(jnp.int32)


def setup_inputs(seed: int = 0) -> dict:
    key_list = jax.random.split(jax.random.key(seed), 8)
    total_tok = DEVICES * TOK_DEV
    tokens = jax.random.normal(key_list[0], (total_tok, D_MODEL), jnp.float32)
    w_one = jax.random.normal(key_list[1], (D_MODEL, D_FF), jnp.float32) * D_MODEL ** -0.5
    w_two = jax.random.normal(key_list[2], (D_FF, D_MODEL), jnp.float32) * D_FF ** -0.5
    adapter_a = jax.random.normal(key_list[3], (D_MODEL, LORA_RANK), jnp.float32) * D_MODEL ** -0.5
    adapter_b = jax.random.normal(key_list[4], (LORA_RANK, D_FF), jnp.float32) * LORA_RANK ** -0.5
    head_common = jax.random.normal(key_list[5], (D_MODEL, NUM_CLASSES), jnp.float32)
    head_own = jax.random.normal(key_list[6], (NUM_TASKS, D_MODEL, NUM_CLASSES), jnp.float32)
    head_sign = jnp.where(jnp.arange(NUM_TASKS) % 2 == 0, 1.0, -1.0)
    task_heads = (head_sign[:, None, None] * head_common[None] + 0.8 * head_own) * (1.5 * D_MODEL ** -0.5)
    labels = draw_labels(key_list[7])
    return {
        "tokens": tokens.astype(jnp.bfloat16),
        "labels": labels,
        "w_one": w_one.astype(jnp.bfloat16),
        "w_two": w_two.astype(jnp.bfloat16),
        "adapter_a": adapter_a.astype(jnp.bfloat16),
        "adapter_b": adapter_b.astype(jnp.bfloat16),
        "task_heads": task_heads.astype(jnp.bfloat16),
    }


def block_grads(tok_blk, lab_blk, w_one, w_two, adapter_a, adapter_b, task_heads):
    low_rank = jnp.dot(tok_blk, adapter_a, preferred_element_type=jnp.float32).astype(jnp.bfloat16)
    pre_act = jnp.dot(tok_blk, w_one, preferred_element_type=jnp.float32) + jnp.dot(low_rank, adapter_b, preferred_element_type=jnp.float32)
    gelu_out, gelu_slope = jax.jvp(jax.nn.gelu, (pre_act,), (jnp.ones_like(pre_act),))
    hidden = gelu_out.astype(jnp.bfloat16)
    trunk_out = (tok_blk.astype(jnp.float32) + jnp.dot(hidden, w_two, preferred_element_type=jnp.float32)).astype(jnp.bfloat16)
    logits = jnp.einsum("bd,tdc->tbc", trunk_out.astype(jnp.float32), task_heads.astype(jnp.float32))
    task_probs = jax.nn.softmax(logits, axis=-1)
    onehot = (lab_blk[:, :, None] == jnp.arange(NUM_CLASSES)[None, None, :]).astype(jnp.float32)
    logit_err = (task_probs - onehot).astype(jnp.bfloat16)
    d_trunk = jnp.einsum("tbc,tdc->tbd", logit_err.astype(jnp.float32), task_heads.astype(jnp.float32)).astype(jnp.bfloat16)
    d_hidden = jnp.einsum("tbd,fd->tbf", d_trunk.astype(jnp.float32), w_two.astype(jnp.float32))
    d_pre = (d_hidden * gelu_slope[None]).astype(jnp.bfloat16)
    part_b = jnp.einsum("br,tbf->trf", low_rank.astype(jnp.float32), d_pre.astype(jnp.float32))
    d_low = jnp.einsum("tbf,rf->tbr", d_pre.astype(jnp.float32), adapter_b.astype(jnp.float32)).astype(jnp.bfloat16)
    part_a = jnp.einsum("bd,tbr->tdr", tok_blk.astype(jnp.float32), d_low.astype(jnp.float32))
    return part_a, part_b


def reference(tokens, labels, w_one, w_two, adapter_a, adapter_b, task_heads):
    tok_blocks = tokens.reshape(DEVICES, TOK_DEV, D_MODEL)
    lab_blocks = labels.reshape(NUM_TASKS, DEVICES, TOK_DEV).transpose(1, 0, 2)

    def add_block(run_sum, block_in):
        part_a, part_b = block_grads(block_in[0], block_in[1], w_one, w_two, adapter_a, adapter_b, task_heads)
        return (run_sum[0] + part_a, run_sum[1] + part_b), None

    zero_init = (jnp.zeros((NUM_TASKS, D_MODEL, LORA_RANK), jnp.float32), jnp.zeros((NUM_TASKS, LORA_RANK, D_FF), jnp.float32))
    sums, _ = lax.scan(add_block, zero_init, (tok_blocks, lab_blocks))
    batch_total = DEVICES * TOK_DEV
    grad_a = sums[0] / batch_total
    grad_b = sums[1] / batch_total
    gram_mat = jnp.einsum("tdr,sdr->ts", grad_a, grad_a) + jnp.einsum("trf,srf->ts", grad_b, grad_b)
    eg_scale = jnp.trace(gram_mat) / NUM_TASKS

    def eg_step(weights, _):
        weights = weights * jnp.exp(-jnp.sum(gram_mat * weights[None, :], axis=1) / eg_scale)
        return weights / jnp.sum(weights), None

    task_weights, _ = lax.scan(eg_step, jnp.full((NUM_TASKS,), 1.0 / NUM_TASKS, jnp.float32), None, length=EG_STEPS)
    comb_a = jnp.sum(task_weights[:, None, None] * grad_a, axis=0)
    comb_b = jnp.sum(task_weights[:, None, None] * grad_b, axis=0)
    return (task_weights, comb_a, comb_b)
```

```python
import functools

import jax
import jax.numpy as jnp
from jax import lax
from jax.experimental import pallas as pl
from jax.experimental.pallas import tpu as pltpu
from jax.sharding import PartitionSpec as P

EG_STEPS = 20
AXIS = "data"
DIMS = (8, 4, 4, 2)
LANES = 128
MESH_ID = pl.DeviceIdType.MESH


def task_grads(tokens, labels, w_one, w_two, adapter_a, adapter_b, task_heads):
    num_classes = task_heads.shape[2]
    low_rank = jnp.dot(tokens, adapter_a, preferred_element_type=jnp.float32).astype(jnp.bfloat16)
    pre_act = jnp.dot(tokens, w_one, preferred_element_type=jnp.float32) + jnp.dot(low_rank, adapter_b, preferred_element_type=jnp.float32)
    gelu_out, gelu_slope = jax.jvp(jax.nn.gelu, (pre_act,), (jnp.ones_like(pre_act),))
    hidden = gelu_out.astype(jnp.bfloat16)
    trunk_out = (tokens.astype(jnp.float32) + jnp.dot(hidden, w_two, preferred_element_type=jnp.float32)).astype(jnp.bfloat16)
    logits = jnp.einsum("bd,tdc->tbc", trunk_out, task_heads, preferred_element_type=jnp.float32)
    task_probs = jax.nn.softmax(logits, axis=-1)
    onehot = (labels[:, :, None] == jnp.arange(num_classes)[None, None, :]).astype(jnp.float32)
    logit_err = (task_probs - onehot).astype(jnp.bfloat16)
    d_trunk = jnp.einsum("tbc,tdc->tbd", logit_err, task_heads, preferred_element_type=jnp.float32).astype(jnp.bfloat16)
    d_hidden = jnp.einsum("tbd,fd->tbf", d_trunk, w_two, preferred_element_type=jnp.float32)
    d_pre = (d_hidden * gelu_slope[None]).astype(jnp.bfloat16)
    part_b = jnp.einsum("cs,ucg->usg", low_rank, d_pre, preferred_element_type=jnp.float32)
    d_low = jnp.einsum("tbf,rf->tbr", d_pre, adapter_b, preferred_element_type=jnp.float32).astype(jnp.bfloat16)
    part_a = jnp.einsum("bd,tbr->trd", tokens, d_low, preferred_element_type=jnp.float32)
    return part_a, part_b


def remote(src, dst, send_sem, recv_sem, dev):
    return pltpu.make_async_remote_copy(src_ref=src, dst_ref=dst, send_sem=send_sem, recv_sem=recv_sem, device_id=(dev,), device_id_type=MESH_ID)


def exchange_kernel(dims, tasks, batch_total, pb_ref, pa_ref, alpha_ref, ga_ref, gb_ref, pk, swap, mine, rs, xs, gram, swap_s, swap_r, rs_s, rs_r, x_s, x_r, g_s, g_r):
    dim_z, dim_y, dim_x, _ = dims
    num_q = dim_z * dim_y
    rank = pb_ref.shape[0] // tasks
    half = pb_ref.shape[0] // 2
    wide_b = pb_ref.shape[1] // num_q
    wide_a = pa_ref.shape[1] // num_q
    own_b = wide_b // (dim_x * 2)
    own_a = wide_a // (dim_x * 2)

    me = lax.axis_index(AXIS)
    core = lax.rem(me, 2)
    x_pos = lax.rem(me // 2, dim_x)
    q_pos = me // (2 * dim_x)
    y_pos = lax.rem(q_pos, dim_y)
    z_pos = q_pos // dim_y

    def dev(q, x, c):
        return (q * dim_x + x) * 2 + c

    offsets = [(dz, dy) for dz in range(dim_z) for dy in range(dim_y)]
    offsets.sort(key=lambda o: -(min(o[0], dim_z - o[0]) + min(o[1], dim_y - o[1])))
    ahead = [lax.rem(z_pos + dz, dim_z) * dim_y + lax.rem(y_pos + dy, dim_y) for dz, dy in offsets]
    partner = dev(q_pos, x_pos, 1 - core)
    row_peers = [(kx, kc) for kx in range(dim_x) for kc in range(2) if (kx, kc) != (0, 0)]

    def row_dev(kx, kc):
        return dev(q_pos, lax.rem(x_pos + kx, dim_x), lax.rem(core + kc, 2))

    barrier = pltpu.get_barrier_semaphore()
    for s in range(num_q - 1):
        pl.semaphore_signal(barrier, inc=1, device_id=(dev(ahead[s], x_pos, core),), device_id_type=MESH_ID)
    for kx, kc in row_peers:
        pl.semaphore_signal(barrier, inc=1, device_id=(row_dev(kx, kc),), device_id_type=MESH_ID)

    for q in range(num_q):
        chunk = jnp.concatenate(
            [
                pb_ref[:, q * wide_b : (q + 1) * wide_b],
                pa_ref[:, q * wide_a : (q + 1) * wide_a],
                jnp.zeros((2 * half, LANES - wide_a - wide_b), jnp.float32),
            ],
            axis=1,
        )
        pk[0, q] = chunk[:half]
        pk[1, q] = chunk[half:]

    pl.semaphore_wait(barrier, num_q - 1 + len(row_peers))

    swaps = [remote(pk.at[1 - core, ahead[s]], swap.at[s], swap_s.at[s], swap_r.at[s], partner) for s in range(num_q)]
    for copy in swaps:
        copy.start()
    sends = []
    for s in range(num_q):
        swaps[s].wait_recv()
        mine[s] = pk[core, ahead[s]] + swap[s]
        if s < num_q - 1:
            copy = remote(mine.at[s], rs.at[s], rs_s.at[s], rs_r.at[s], dev(ahead[s], x_pos, core))
            copy.start()
            sends.append(copy)
    acc = mine[num_q - 1]
    for s in reversed(range(num_q - 1)):
        sends[s].wait_recv()
        acc = acc + rs[s]

    xs[core, x_pos] = acc
    for i, (kx, kc) in enumerate(row_peers):
        copy = remote(xs.at[core, x_pos], xs.at[core, x_pos], x_s.at[i], x_r.at[core, x_pos], row_dev(kx, kc))
        copy.start()
        sends.append(copy)
    for i, (kx, kc) in enumerate(row_peers):
        cc, xx = lax.rem(core + kc, 2), lax.rem(x_pos + kx, dim_x)
        remote(xs.at[cc, xx], xs.at[cc, xx], x_s.at[i], x_r.at[cc, xx], row_dev(kx, kc)).wait_recv()
    grads = []
    for c in range(2):
        both = xs[c, 0]
        for i in range(1, dim_x):
            both = both + xs[c, i]
        both = both * (1.0 / batch_total)
        for t in range(tasks // 2):
            grads.append(both[t * rank : (t + 1) * rank])

    lane = lax.broadcasted_iota(jnp.int32, (1, LANES), 1)
    pairs = [(t, s) for t in range(tasks) for s in range(t, tasks)]
    row = jnp.zeros((1, LANES), jnp.float32)
    for i, (t, s) in enumerate(pairs):
        dot = jnp.sum(jnp.sum(grads[t] * grads[s], axis=0, keepdims=True), axis=1, keepdims=True)
        row = jnp.where(lane == i, dot, row)
    gram[q_pos] = row
    for s in range(num_q - 1):
        copy = remote(gram.at[q_pos], gram.at[q_pos], g_s.at[s], g_r.at[q_pos], dev(ahead[s], x_pos, core))
        copy.start()
        sends.append(copy)
    for s in range(num_q - 1):
        remote(gram.at[ahead[s]], gram.at[ahead[s]], g_s.at[s], g_r.at[ahead[s]], dev(ahead[s], x_pos, core)).wait_recv()
    row = gram[0]
    for q in range(1, num_q):
        row = row + gram[q]
    mat = {}
    for i, (t, s) in enumerate(pairs):
        val = jnp.sum(jnp.where(lane == i, row, 0.0), axis=1, keepdims=True)
        mat[t, s] = mat[s, t] = jnp.broadcast_to(val, (1, LANES))
    scale = mat[0, 0]
    for t in range(1, tasks):
        scale = scale + mat[t, t]
    scale = scale / tasks
    weights = tuple(jnp.full((1, LANES), 1.0 / tasks, jnp.float32) for _ in range(tasks))

    def eg_step(_, weights):
        new = []
        for t in range(tasks):
            dot = mat[t, 0] * weights[0]
            for s in range(1, tasks):
                dot = dot + mat[t, s] * weights[s]
            new.append(weights[t] * jnp.exp(-dot / scale))
        total = new[0]
        for t in range(1, tasks):
            total = total + new[t]
        return tuple(w / total for w in new)

    weights = lax.fori_loop(0, EG_STEPS, eg_step, weights)
    row = jnp.zeros((1, LANES), jnp.float32)
    comb = jnp.zeros((rank, LANES), jnp.float32)
    for t in range(tasks):
        row = jnp.where(lane == t, weights[t], row)
        comb = comb + weights[t] * grads[t]
    alpha_ref[...] = row[:, :tasks]
    place = x_pos * 2 + core
    gb_ref[...] = pltpu.roll(comb, lax.rem(LANES - place * own_b, LANES), 1)[:, :own_b]
    ga_ref[...] = jnp.transpose(pltpu.roll(comb, LANES - wide_b - place * own_a, 1))[:own_a]
    for copy in swaps + sends:
        copy.wait_send()


def exchange(part_b, part_a, dims, tasks, batch_total):
    num_dev = 2 * dims[0] * dims[1] * dims[2]
    num_q = dims[0] * dims[1]
    rank = part_b.shape[0] // tasks
    half = part_b.shape[0] // 2
    slab = (half, LANES)
    dma = pltpu.SemaphoreType.DMA
    return pl.pallas_call(
        functools.partial(exchange_kernel, dims, tasks, batch_total),
        out_shape=(
            jax.ShapeDtypeStruct((1, tasks), jnp.float32),
            jax.ShapeDtypeStruct((part_a.shape[1] // num_dev, rank), jnp.float32),
            jax.ShapeDtypeStruct((rank, part_b.shape[1] // num_dev), jnp.float32),
        ),
        in_specs=[pl.BlockSpec(memory_space=pltpu.VMEM)] * 2,
        out_specs=[pl.BlockSpec(memory_space=pltpu.VMEM)] * 3,
        scratch_shapes=[
            pltpu.VMEM((2, num_q) + slab, jnp.float32),
            pltpu.VMEM((num_q,) + slab, jnp.float32),
            pltpu.VMEM((num_q,) + slab, jnp.float32),
            pltpu.VMEM((num_q,) + slab, jnp.float32),
            pltpu.VMEM((2, dims[2]) + slab, jnp.float32),
            pltpu.VMEM((num_q, 1, LANES), jnp.float32),
            dma((num_q,)),
            dma((num_q,)),
            dma((num_q,)),
            dma((num_q,)),
            dma((2 * dims[2],)),
            dma((2, dims[2])),
            dma((num_q,)),
            dma((num_q,)),
        ],
        compiler_params=pltpu.CompilerParams(collective_id=0, has_side_effects=True),
        name="exchange",
    )(part_b, part_a)


def solution(mesh):
    num_dev = mesh.shape[AXIS]

    def device_step(tokens, labels, w_one, w_two, adapter_a, adapter_b, task_heads):
        batch_total = tokens.shape[0] * num_dev
        tasks = task_heads.shape[0]
        part_a, part_b = task_grads(tokens, labels, w_one, w_two, adapter_a, adapter_b, task_heads)
        part_a = part_a.reshape(-1, part_a.shape[2])
        part_b = part_b.reshape(-1, part_b.shape[2])
        alpha, grad_a, grad_b = exchange(part_b, part_a, DIMS, tasks, batch_total)
        return alpha.reshape(tasks), grad_a, grad_b

    return jax.shard_map(device_step, mesh=mesh, in_specs=(P(AXIS, None), P(None, AXIS), P(), P(), P(), P(), P()), out_specs=(P(), P(AXIS, None), P(None, AXIS)), check_vma=False)
```

```python
import functools

import jax
import jax.numpy as jnp
from jax import lax
from jax.experimental import pallas as pl
from jax.experimental.pallas import tpu as pltpu
from jax.sharding import PartitionSpec as P

EG_STEPS = 20
AXIS = "data"
DIMS = (8, 4, 4, 2)
LANES = 128
MESH_ID = pl.DeviceIdType.MESH


F32, BF16 = jnp.float32, jnp.bfloat16
NT = (((1,), (1,)), ((), ()))
TN = (((0,), (0,)), ((), ()))
ROOT = 0.7978845608028654
CUBE = 0.044715


def dot(a, b, dims=(((1,), (0,)), ((), ()))):
    return lax.dot_general(a, b, dims, preferred_element_type=F32)


def compute_kernel(nb1, nb3, grp, x_hbm, lab_hbm, w1_hbm, w2_hbm, a_hbm, bm_hbm, hd_hbm, pb_ref, pa_ref, x, lab, w1, w2, a, bm, hd, h, slope, dz, ut, sem, sem1, sem2):
    num_tok, d_model = x.shape
    d_ff = h.shape[1]
    tasks, _, classes = hd.shape
    rank = bm.shape[0]
    n1, n3 = d_ff // nb1, d_ff // nb3
    small = [(x_hbm, x), (a_hbm, a), (bm_hbm, bm)]
    late = [(hd_hbm, hd), (lab_hbm, lab)]
    first = [pltpu.make_async_copy(s, d, sem.at[i]) for i, (s, d) in enumerate(small)]
    col = [pltpu.make_async_copy(w1_hbm.at[:, i * nb1 : (i + 1) * nb1], w1.at[i], sem1.at[i]) for i in range(n1)]
    row = [pltpu.make_async_copy(w2_hbm.at[i * nb1 : (i + 1) * nb1], w2.at[i * nb1 : (i + 1) * nb1], sem2.at[i]) for i in range(n1)]
    last = [pltpu.make_async_copy(s, d, sem.at[3 + i]) for i, (s, d) in enumerate(late)]
    for c in first + col + last + row:
        c.start()
    for c in first:
        c.wait()
    xv = x[...]
    low = dot(xv, a[...])
    u = low.astype(BF16)
    ut[...] = jnp.transpose(low).astype(BF16)

    def forward(i, carry):
        pltpu.make_async_copy(w1_hbm.at[:, pl.ds(pl.multiple_of(i * nb1, nb1), nb1)], w1.at[i], sem1.at[i]).wait()
        cols = pl.ds(pl.multiple_of(i * nb1, nb1), nb1)
        p = dot(x[...], w1[i]) + dot(u, bm[:, cols])
        sq = p * p
        t = jnp.tanh(ROOT * p * (1.0 + CUBE * sq))
        cdf = 0.5 + 0.5 * t
        h[:, cols] = (p * cdf).astype(BF16)
        slope[:, cols] = cdf + (0.5 * p) * (1.0 - t * t) * (ROOT + (3.0 * CUBE * ROOT) * sq)
        return carry

    lax.fori_loop(0, n1, forward, 0)
    for c in row + last:
        c.wait()
    z = (x[...].astype(F32) + dot(h[...], w2[...])).astype(BF16)
    per_task = [jnp.transpose(hd[t].astype(F32)) for t in range(tasks)]
    head_rows = jnp.concatenate([per_task[t][c : c + 1] for c in range(classes) for t in range(tasks)], axis=0)
    heads = head_rows.astype(BF16)
    logits = dot(heads, z, NT)
    cls = [logits[c * tasks : (c + 1) * tasks] for c in range(classes)]
    top = functools.reduce(jnp.maximum, cls)
    ex = [jnp.exp(v - top) for v in cls]
    tot = functools.reduce(jnp.add, ex)
    labels = lab[...]
    err = jnp.concatenate([e / tot - (labels == c).astype(F32) for c, e in enumerate(ex)], axis=0)
    err = jnp.transpose(err).astype(BF16)
    own = lax.rem(lax.broadcasted_iota(jnp.int32, head_rows.shape, 0), tasks)
    for t in range(tasks):
        dz[t * num_tok : (t + 1) * num_tok] = dot(err, jnp.where(own == t, head_rows, 0.0).astype(BF16)).astype(BF16)

    def backward(i, dlow):
        cols = pl.ds(pl.multiple_of(i * nb3, nb3), nb3)
        wb = w2[cols, :]
        sl = slope[:, cols]
        new = []
        for g in range(0, tasks, grp):
            dh = dot(dz[g * num_tok : (g + grp) * num_tok], wb, NT)
            for t in range(g, g + grp):
                dp = (dh[(t - g) * num_tok : (t - g + 1) * num_tok] * sl).astype(BF16)
                pb_ref[pl.ds(t * rank, rank), cols] = dot(ut[...], dp)
                new.append(dlow[t] + dot(bm[:, cols], dp, NT))
        return tuple(new)

    dlow = lax.fori_loop(0, n3, backward, tuple(jnp.zeros((rank, num_tok), F32) for _ in range(tasks)))
    pa_ref[...] = dot(jnp.concatenate(dlow, axis=0).astype(BF16), x[...])


def local_grads(tokens, labels, w_one, w_two, adapter_a, adapter_b, task_heads, nb1=1536, nb3=1536, grp=2):
    num_tok, d_model = tokens.shape
    d_ff = w_one.shape[1]
    tasks, _, classes = task_heads.shape
    rank = adapter_b.shape[0]
    dma = pltpu.SemaphoreType.DMA
    n1 = d_ff // nb1
    return pl.pallas_call(
        functools.partial(compute_kernel, nb1, nb3, grp),
        out_shape=(jax.ShapeDtypeStruct((tasks * rank, d_ff), F32), jax.ShapeDtypeStruct((tasks * rank, d_model), F32)),
        in_specs=[pl.BlockSpec(memory_space=pl.ANY)] * 7,
        out_specs=[pl.BlockSpec(memory_space=pltpu.VMEM)] * 2,
        scratch_shapes=[
            pltpu.VMEM(tokens.shape, BF16),
            pltpu.VMEM(labels.shape, jnp.int32),
            pltpu.VMEM((n1, d_model, nb1), BF16),
            pltpu.VMEM(w_two.shape, BF16),
            pltpu.VMEM(adapter_a.shape, BF16),
            pltpu.VMEM(adapter_b.shape, BF16),
            pltpu.VMEM(task_heads.shape, BF16),
            pltpu.VMEM((num_tok, d_ff), BF16),
            pltpu.VMEM((num_tok, d_ff), F32),
            pltpu.VMEM((tasks * num_tok, d_model), BF16),
            pltpu.VMEM((rank, num_tok), BF16),
            dma((5,)),
            dma((n1,)),
            dma((n1,)),
        ],
        name="local_grads",
    )(tokens, labels, w_one, w_two, adapter_a, adapter_b, task_heads)


def remote(src, dst, send_sem, recv_sem, dev):
    return pltpu.make_async_remote_copy(src_ref=src, dst_ref=dst, send_sem=send_sem, recv_sem=recv_sem, device_id=(dev,), device_id_type=MESH_ID)


def exchange_kernel(dims, tasks, batch_total, pb_ref, pa_ref, alpha_ref, ga_ref, gb_ref, pk, swap, mine, rs, xs, gram, swap_s, swap_r, rs_s, rs_r, x_s, x_r, g_s, g_r):
    dim_z, dim_y, dim_x, _ = dims
    num_q = dim_z * dim_y
    rank = pb_ref.shape[0] // tasks
    half = pb_ref.shape[0] // 2
    wide_b = pb_ref.shape[1] // num_q
    wide_a = pa_ref.shape[1] // num_q
    own_b = wide_b // (dim_x * 2)
    own_a = wide_a // (dim_x * 2)

    me = lax.axis_index(AXIS)
    core = lax.rem(me, 2)
    x_pos = lax.rem(me // 2, dim_x)
    q_pos = me // (2 * dim_x)
    y_pos = lax.rem(q_pos, dim_y)
    z_pos = q_pos // dim_y

    def dev(q, x, c):
        return (q * dim_x + x) * 2 + c

    offsets = [(dz, dy) for dz in range(dim_z) for dy in range(dim_y)]
    offsets.sort(key=lambda o: -(min(o[0], dim_z - o[0]) + min(o[1], dim_y - o[1])))
    ahead = [lax.rem(z_pos + dz, dim_z) * dim_y + lax.rem(y_pos + dy, dim_y) for dz, dy in offsets]
    partner = dev(q_pos, x_pos, 1 - core)
    row_peers = [(kx, kc) for kx in range(dim_x) for kc in range(2) if (kx, kc) != (0, 0)]

    def row_dev(kx, kc):
        return dev(q_pos, lax.rem(x_pos + kx, dim_x), lax.rem(core + kc, 2))

    barrier = pltpu.get_barrier_semaphore()
    for s in range(num_q - 1):
        pl.semaphore_signal(barrier, inc=1, device_id=(dev(ahead[s], x_pos, core),), device_id_type=MESH_ID)
    for kx, kc in row_peers:
        pl.semaphore_signal(barrier, inc=1, device_id=(row_dev(kx, kc),), device_id_type=MESH_ID)

    for q in range(num_q):
        chunk = jnp.concatenate(
            [
                pb_ref[:, q * wide_b : (q + 1) * wide_b],
                pa_ref[:, q * wide_a : (q + 1) * wide_a],
                jnp.zeros((2 * half, LANES - wide_a - wide_b), jnp.float32),
            ],
            axis=1,
        )
        pk[0, q] = chunk[:half]
        pk[1, q] = chunk[half:]

    pl.semaphore_wait(barrier, num_q - 1 + len(row_peers))

    swaps = [remote(pk.at[1 - core, ahead[s]], swap.at[s], swap_s.at[s], swap_r.at[s], partner) for s in range(num_q)]
    for copy in swaps:
        copy.start()
    sends = []
    for s in range(num_q):
        swaps[s].wait_recv()
        mine[s] = pk[core, ahead[s]] + swap[s]
        if s < num_q - 1:
            copy = remote(mine.at[s], rs.at[s], rs_s.at[s], rs_r.at[s], dev(ahead[s], x_pos, core))
            copy.start()
            sends.append(copy)
    acc = mine[num_q - 1]
    for s in reversed(range(num_q - 1)):
        sends[s].wait_recv()
        acc = acc + rs[s]

    xs[core, x_pos] = acc
    for i, (kx, kc) in enumerate(row_peers):
        copy = remote(xs.at[core, x_pos], xs.at[core, x_pos], x_s.at[i], x_r.at[core, x_pos], row_dev(kx, kc))
        copy.start()
        sends.append(copy)
    for i, (kx, kc) in enumerate(row_peers):
        cc, xx = lax.rem(core + kc, 2), lax.rem(x_pos + kx, dim_x)
        remote(xs.at[cc, xx], xs.at[cc, xx], x_s.at[i], x_r.at[cc, xx], row_dev(kx, kc)).wait_recv()
    grads = []
    for c in range(2):
        both = xs[c, 0]
        for i in range(1, dim_x):
            both = both + xs[c, i]
        both = both * (1.0 / batch_total)
        for t in range(tasks // 2):
            grads.append(both[t * rank : (t + 1) * rank])

    lane = lax.broadcasted_iota(jnp.int32, (1, LANES), 1)
    pairs = [(t, s) for t in range(tasks) for s in range(t, tasks)]
    row = jnp.zeros((1, LANES), jnp.float32)
    for i, (t, s) in enumerate(pairs):
        dot = jnp.sum(jnp.sum(grads[t] * grads[s], axis=0, keepdims=True), axis=1, keepdims=True)
        row = jnp.where(lane == i, dot, row)
    gram[q_pos] = row
    for s in range(num_q - 1):
        copy = remote(gram.at[q_pos], gram.at[q_pos], g_s.at[s], g_r.at[q_pos], dev(ahead[s], x_pos, core))
        copy.start()
        sends.append(copy)
    for s in range(num_q - 1):
        remote(gram.at[ahead[s]], gram.at[ahead[s]], g_s.at[s], g_r.at[ahead[s]], dev(ahead[s], x_pos, core)).wait_recv()
    row = gram[0]
    for q in range(1, num_q):
        row = row + gram[q]
    mat = {}
    for i, (t, s) in enumerate(pairs):
        val = jnp.sum(jnp.where(lane == i, row, 0.0), axis=1, keepdims=True)
        mat[t, s] = mat[s, t] = jnp.broadcast_to(val, (1, LANES))
    scale = mat[0, 0]
    for t in range(1, tasks):
        scale = scale + mat[t, t]
    scale = scale / tasks
    weights = tuple(jnp.full((1, LANES), 1.0 / tasks, jnp.float32) for _ in range(tasks))

    def eg_step(_, weights):
        new = []
        for t in range(tasks):
            dot = mat[t, 0] * weights[0]
            for s in range(1, tasks):
                dot = dot + mat[t, s] * weights[s]
            new.append(weights[t] * jnp.exp(-dot / scale))
        total = new[0]
        for t in range(1, tasks):
            total = total + new[t]
        return tuple(w / total for w in new)

    weights = lax.fori_loop(0, EG_STEPS, eg_step, weights)
    row = jnp.zeros((1, LANES), jnp.float32)
    comb = jnp.zeros((rank, LANES), jnp.float32)
    for t in range(tasks):
        row = jnp.where(lane == t, weights[t], row)
        comb = comb + weights[t] * grads[t]
    alpha_ref[...] = row[:, :tasks]
    place = x_pos * 2 + core
    gb_ref[...] = pltpu.roll(comb, lax.rem(LANES - place * own_b, LANES), 1)[:, :own_b]
    ga_ref[...] = jnp.transpose(pltpu.roll(comb, LANES - wide_b - place * own_a, 1))[:own_a]
    for copy in swaps + sends:
        copy.wait_send()


def exchange(part_b, part_a, dims, tasks, batch_total):
    num_dev = 2 * dims[0] * dims[1] * dims[2]
    num_q = dims[0] * dims[1]
    rank = part_b.shape[0] // tasks
    half = part_b.shape[0] // 2
    slab = (half, LANES)
    dma = pltpu.SemaphoreType.DMA
    return pl.pallas_call(
        functools.partial(exchange_kernel, dims, tasks, batch_total),
        out_shape=(
            jax.ShapeDtypeStruct((1, tasks), jnp.float32),
            jax.ShapeDtypeStruct((part_a.shape[1] // num_dev, rank), jnp.float32),
            jax.ShapeDtypeStruct((rank, part_b.shape[1] // num_dev), jnp.float32),
        ),
        in_specs=[pl.BlockSpec(memory_space=pltpu.VMEM)] * 2,
        out_specs=[pl.BlockSpec(memory_space=pltpu.VMEM)] * 3,
        scratch_shapes=[
            pltpu.VMEM((2, num_q) + slab, jnp.float32),
            pltpu.VMEM((num_q,) + slab, jnp.float32),
            pltpu.VMEM((num_q,) + slab, jnp.float32),
            pltpu.VMEM((num_q,) + slab, jnp.float32),
            pltpu.VMEM((2, dims[2]) + slab, jnp.float32),
            pltpu.VMEM((num_q, 1, LANES), jnp.float32),
            dma((num_q,)),
            dma((num_q,)),
            dma((num_q,)),
            dma((num_q,)),
            dma((2 * dims[2],)),
            dma((2, dims[2])),
            dma((num_q,)),
            dma((num_q,)),
        ],
        compiler_params=pltpu.CompilerParams(collective_id=0, has_side_effects=True),
        name="exchange",
    )(part_b, part_a)


def solution(mesh):
    num_dev = mesh.shape[AXIS]

    def device_step(tokens, labels, w_one, w_two, adapter_a, adapter_b, task_heads):
        batch_total = tokens.shape[0] * num_dev
        tasks = task_heads.shape[0]
        part_b, part_a = local_grads(tokens, labels, w_one, w_two, adapter_a, adapter_b, task_heads)
        alpha, grad_a, grad_b = exchange(part_b, part_a, DIMS, tasks, batch_total)
        return alpha.reshape(tasks), grad_a, grad_b

    return jax.shard_map(device_step, mesh=mesh, in_specs=(P(AXIS, None), P(None, AXIS), P(), P(), P(), P(), P()), out_specs=(P(), P(AXIS, None), P(None, AXIS)), check_vma=False)
```
